32 devices in a mesh: dp: 2 (over y), expert: 16 (over z, x, core).
Axes of the slice: x: 2, y: 2, z: 4, core: 2. Of those that a mesh axis runs over, the one named last changes fastest.
Arguments:
- tokens: bfloat16 [256, 2880], P(('dp', 'expert')), may hold values from -6 to 6
- routes: int32 [2, 256, 4], P(None, ('dp', 'expert')), may hold values from 0 to 15, all different within a row; in each aligned block of 8 rows (0 to 7, 8 to 15, ..., all dimensions but the last counted through in order) at most 4 rows name the same one
- placement: int32 [2, 16], replicated, may hold values from 0 to 15, each once within a row
- up_weight: bfloat16 [2, 16, 2880, 1440], P(None, 'expert', None, 'dp'), may hold values from -0.109375 to 0.109375
- down_weight: bfloat16 [2, 16, 1440, 2880], P(None, 'expert', 'dp'), may hold values from -0.15625 to 0.15625
- router_weight: bfloat16 [2, 16, 2880], P(None, 'expert'), may hold values from -0.21875 to 0.21875
Outputs:
- final_stream: bfloat16 [256, 2880], P(('dp', 'expert'))
The draws below stay inside these ranges and needn't reach their ends.
Inputs may be any that keep to these rules, and one draw needn't show every extreme that they name: `routes`: each row names 4 different experts. Within one layer's rows of one device no expert is named by more than 4 rows, and some device names some expert exactly 4 times. `placement`: each layer's row is a permutation of the slots.
All inputs are finite; a program needn't handle non-finite values.
Results may differ from the reference program's by a relative error of at most 0.008.
Values may be sent and summed in bfloat16 or wider, within the bound.
No kernel may reach another device: no remote copies, remote signals or barrier semaphores. Data moves between devices by JAX's collectives and lax.ppermute only.
A program may use at most 64 MiB of HBM per device.

```python
import math
import jax
import jax.numpy as jnp
import numpy as np
from jax import lax

D = 2880
TOPK = 4
FF = 1440
LAYERS = 2
TOK_DEV = 8
EXPERTS = 16
FF_DEV = 720
CAP = 4
TOKENS = 256
N_DP = 2
N_EXPERT = 16


def levels(stream_key, extent, split, least, largest):
    factor_of, own = 1.0, jax.random.fold_in(stream_key, 6)
    for position, parts in split:
        heights = jnp.exp(jax.random.uniform(jax.random.fold_in(own, position), (parts,), jnp.float32, least / len(split), largest / len(split)))
        factor_of = factor_of * jnp.repeat(heights, extent[position] // parts).reshape([-1 if axis == position else 1 for axis in range(len(extent))])
    return factor_of


def assign_block(own_key, own, number, rows, count, top, reach, slope):
    ranking = jax.random.permutation(own_key, count)
    crowded, usual = load_shares(count, rows * top, reach, slope, True), load_shares(count, rows * top, reach, slope, False)
    places = jnp.arange(count)

    def named(sizes, rotation):
        used = int((sizes > 0).sum())
        fixed = max(1, used // 4)
        moved = fixed + (places - fixed + rotation * (used - fixed)) % max(1, count - fixed)
        return jnp.zeros((count,), jnp.int32).at[ranking[jnp.where(places < fixed, places, moved)]].set(jnp.asarray(sizes, jnp.int32))

    sizes = jnp.where(number % 4 == 0, named(crowded, number // 4), named(usual, number - number // 4 - 1))
    mixed = jax.random.permutation(jax.random.fold_in(own, 3), count)
    giver, receiver = mixed[0:count // 2 * 2:2], mixed[1:count // 2 * 2:2]
    room = jnp.minimum(sizes[giver] - 1, reach - sizes[receiver]) // 2
    room = jnp.where((giver == ranking[0]) | (receiver == ranking[0]) | (sizes[receiver] == 0), 0, jnp.maximum(room, 0))
    moved = jax.random.randint(jax.random.fold_in(own, 4), (count // 2,), 0, 1 << 20) % (room + 1)
    sizes = sizes.at[giver].add(-moved).at[receiver].add(moved)
    items = jnp.searchsorted(jnp.cumsum(sizes), jnp.arange(rows * top), side="right").astype(jnp.int32)
    listing = items.reshape(top, rows).T
    listing = listing[jax.random.permutation(jax.random.fold_in(own, 1), rows)]
    rotation = jax.random.randint(jax.random.fold_in(own, 2), (rows, 1), 0, top)
    return jnp.take_along_axis(listing, (jnp.arange(top)[None, :] + rotation) % top, axis=1)


def load_shares(count, total, reach, slope, full):
    portions = [(1 << 20) // math.isqrt(rank ** slope) + 1 for rank in range(1, count + 1)]
    largest = reach if full else min(reach, max(-(-total // count), total * portions[0] // sum(portions)))
    least = 1 if total - largest >= count - 1 else 0
    holding, spare = [largest] + [least] * (count - 1), total - largest - least * (count - 1)
    while spare > 0:
        movable = [i for i in range(1, count) if holding[i] < largest] or [i for i in range(1, count) if holding[i] < reach]
        whole, budget = sum([portions[i] for i in movable]), spare
        for i in movable:
            extra = min(reach - holding[i], max(1, budget * portions[i] // whole), spare)
            holding[i] = holding[i] + extra
            spare = spare - extra
    return np.array(holding)


def bell_draw(key, extent, width, most, split=(), kind=jnp.bfloat16):
    entries = width * jax.random.normal(key, extent, jnp.float32)
    if split:
        entries = entries * levels(key, extent, split, -0.22, 0.18)
    return jnp.clip(entries, -most, most).astype(kind)


def setup_inputs(seed: int = 0) -> dict:
    splits = jax.random.split(jax.random.key(seed), 7)
    tokens = bell_draw(splits[0], (TOKENS, D), 1.0, 6.0, ((0, 32),))
    routes_keys = jax.random.split(jax.random.fold_in(splits[1], 1), LAYERS * TOKENS // TOK_DEV)
    routes_turns = jax.random.permutation(jax.random.fold_in(splits[1], 3), LAYERS * TOKENS // TOK_DEV)
    routes = jax.vmap(lambda own, number: assign_block(jax.random.fold_in(splits[1], 2), own, number, TOK_DEV, EXPERTS, TOPK, CAP, 1))(routes_keys, routes_turns).reshape((LAYERS, TOKENS, TOPK))
    placement = jax.vmap(lambda own: jax.random.permutation(own, EXPERTS))(jax.random.split(splits[2], LAYERS)).reshape((LAYERS, EXPERTS)).astype(jnp.int32)
    up_weight = bell_draw(splits[3], (LAYERS, EXPERTS, D, FF), D ** -0.5, 0.109375, ((1, 16), (3, 2)))
    down_weight = bell_draw(splits[4], (LAYERS, EXPERTS, FF, D), FF ** -0.5, 0.15625, ((1, 16), (2, 2)))
    router_weight = bell_draw(splits[5], (LAYERS, EXPERTS, D), (D // 4) ** -0.5, 0.21875, ((1, 16),))
    return dict(tokens=tokens, routes=routes, placement=placement, up_weight=up_weight, down_weight=down_weight, router_weight=router_weight)


def rms_rows(stream):
    values = stream.astype(jnp.float32)
    inverse = lax.rsqrt(lax.optimization_barrier(jnp.mean(values * values, axis=-1, keepdims=True)) + 1e-05)
    return (values * inverse).astype(jnp.bfloat16)

def layer_step(stream, packed):
    route_rows, place_row, up_layer, down_layer, router_layer = packed
    normed = rms_rows(stream)
    target = place_row[route_rows].reshape(-1).astype(jnp.int32)
    row_order = jnp.argsort(target, stable=True).astype(jnp.int32)
    sorted_target = target[row_order]
    slot_ids = jnp.arange(EXPERTS, dtype=jnp.int32)
    counts = lax.optimization_barrier(jnp.sum((target[:, None] == slot_ids[None, :]).astype(jnp.int32), axis=0))
    starts = (jnp.cumsum(counts) - counts).astype(jnp.int32)
    slot_rows = N_DP * N_EXPERT * CAP
    picked = jnp.concatenate([normed[row_order // TOPK], jnp.zeros((slot_rows, D), jnp.bfloat16)], axis=0)

    def per_slot(slot_index):
        slot_in = lax.dynamic_slice_in_dim(picked, starts[slot_index], slot_rows, 0)
        hidden = jax.nn.silu(jnp.dot(slot_in, up_layer[slot_index], preferred_element_type=jnp.float32)).astype(jnp.bfloat16)
        blocks = hidden.astype(jnp.float32).reshape(slot_rows, N_DP, FF_DEV)
        down_blocks = down_layer[slot_index].astype(jnp.float32).reshape(N_DP, FF_DEV, D)
        part_sums = jnp.einsum('rbf,bfd->rbd', blocks, down_blocks).astype(jnp.bfloat16)
        output = lax.optimization_barrier(jnp.sum(part_sums.astype(jnp.float32), axis=1))
        affinity = jax.nn.sigmoid(jnp.dot(slot_in, router_layer[slot_index], preferred_element_type=jnp.float32)).astype(jnp.bfloat16)
        return (output, affinity)
    outputs, affinity = lax.map(per_slot, slot_ids)
    within = jnp.arange(target.shape[0], dtype=jnp.int32) - starts[sorted_target]
    sorted_out = outputs[sorted_target, within]
    sorted_gate = affinity[sorted_target, within]
    row_out = jnp.zeros_like(sorted_out).at[row_order].set(sorted_out).reshape(-1, TOPK, D)
    row_gate = jnp.zeros_like(sorted_gate).at[row_order].set(sorted_gate).reshape(-1, TOPK).astype(jnp.float32)
    numerator = lax.optimization_barrier(jnp.sum(row_gate[:, :, None] * row_out, axis=1))
    denominator = jnp.maximum(lax.optimization_barrier(jnp.sum(row_gate, axis=1)), 0.5)
    updated = stream.astype(jnp.float32) + numerator / denominator[:, None]
    return (updated.astype(jnp.bfloat16), None)

def reference(tokens, routes, placement, up_weight, down_weight, router_weight):
    result_stream, unused = lax.scan(layer_step, tokens, (routes, placement, up_weight, down_weight, router_weight))
    return result_stream
```

```python
import functools

import jax
import jax.numpy as jnp
from jax import lax
from jax.experimental import pallas as pl
from jax.experimental.pallas import tpu as pltpu
from jax.sharding import PartitionSpec as P

LANES = 128


def rms_rows(stream):
    values = stream.astype(jnp.float32)
    inverse = lax.rsqrt(jnp.mean(values * values, axis=-1, keepdims=True) + 1e-05)
    return (values * inverse).astype(jnp.bfloat16)


def round_up(value, unit):
    return -(-value // unit) * unit


def column_blocks(extent, step):
    return [(start, min(step, extent - start)) for start in range(0, extent, step)]


def ffn_kernel(layer, width, up_blocks, down_blocks, ids_ref, near_ref, far_ref, router_ref, up_hbm, down_hbm, near_out, far_out, rows_ref, hidden_ref, *scratch):
    up_parts, down_parts = scratch[: len(up_blocks)], scratch[len(up_blocks) : -1]
    sems = scratch[-1]
    copies = []
    for index, (start, size) in enumerate(up_blocks):
        copies.append(pltpu.make_async_copy(up_hbm.at[layer, 0, :, pl.ds(start, size)], up_parts[index], sems.at[index]))
    for index, (start, size) in enumerate(down_blocks):
        copies.append(
            pltpu.make_async_copy(down_hbm.at[layer, 0, :, pl.ds(start, size)], down_parts[index], sems.at[len(up_blocks) + index])
        )
    for copy in copies:
        copy.start()
    half = near_ref.shape[0]
    model = router_ref.shape[-1]
    rows_ref[:half, :] = near_ref[...]
    rows_ref[half:, :] = far_ref[...]
    slot, block = ids_ref[0], ids_ref[1]
    tail = model // LANES * LANES
    lane = lax.broadcasted_iota(jnp.int32, (2 * half, width - tail), 1)
    here = lane == (model - tail) + slot
    member = jnp.sum(jnp.where(here, rows_ref[:, tail:].astype(jnp.float32), 0.0), axis=1, keepdims=True)
    router = router_ref[layer].astype(jnp.float32)
    logits = jnp.sum(rows_ref[:, :model].astype(jnp.float32) * router, axis=1, keepdims=True)
    gate = jax.nn.sigmoid(logits).astype(jnp.bfloat16).astype(jnp.float32) * member
    for index, (start, size) in enumerate(up_blocks):
        copies[index].wait()
        raw = jnp.dot(rows_ref[:, :model], up_parts[index][...], preferred_element_type=jnp.float32)
        hidden_ref[:, start : start + size] = jax.nn.silu(raw).astype(jnp.bfloat16)
    for index, (start, size) in enumerate(down_blocks):
        copies[len(up_blocks) + index].wait()
        part = jnp.dot(hidden_ref[...], down_parts[index][...], preferred_element_type=jnp.float32)
        weighted = (part.astype(jnp.bfloat16).astype(jnp.float32) * gate).astype(jnp.bfloat16)
        near_out[:, start : start + size] = weighted[:half]
        far_out[:, start : start + size] = weighted[half:]
    sent = jnp.where(here & (block == 0), gate, 0.0)[:, model - tail :].astype(jnp.bfloat16)
    near_out[:, model:] = sent[:half]
    far_out[:, model:] = sent[half:]


def expert_ffn(layer, ids, near, far, router, up, down):
    half, width = near.shape
    model, units = up.shape[2], up.shape[3]
    up_blocks = column_blocks(units, 256)
    down_blocks = column_blocks(model, 768)
    scratch = [pltpu.VMEM((2 * half, width), jnp.bfloat16), pltpu.VMEM((2 * half, units), jnp.bfloat16)]
    scratch += [pltpu.VMEM((model, size), jnp.bfloat16) for _, size in up_blocks]
    scratch += [pltpu.VMEM((units, size), jnp.bfloat16) for _, size in down_blocks]
    scratch += [pltpu.SemaphoreType.DMA((len(up_blocks) + len(down_blocks),))]
    vmem = pl.BlockSpec(memory_space=pltpu.VMEM)
    return pl.pallas_call(
        functools.partial(ffn_kernel, layer, width, up_blocks, down_blocks),
        out_shape=[jax.ShapeDtypeStruct((half, width), jnp.bfloat16)] * 2,
        in_specs=[
            pl.BlockSpec(memory_space=pltpu.SMEM),
            vmem,
            vmem,
            vmem,
            pl.BlockSpec(memory_space=pl.ANY),
            pl.BlockSpec(memory_space=pl.ANY),
        ],
        out_specs=[vmem, vmem],
        scratch_shapes=scratch,
        compiler_params=pltpu.CompilerParams(vmem_limit_bytes=32 * 1024 * 1024),
        name=f"ffn_{layer}",
    )(ids, near, far, router, up, down)


def dense_moves(groups, columns):
    lengths = columns // 4

    def pairs(move):
        listed = []
        for group in range(groups):
            for far in range(lengths):
                for side in range(2):
                    for core in range(2):
                        to = move(group, far, side, core)
                        listed.append((((group * lengths + far) * 2 + side) * 2 + core, ((to[0] * lengths + to[1]) * 2 + to[2]) * 2 + to[3]))
        return listed

    def axis_swap(which):
        def move(group, far, side, core):
            return (group, far, 1 - side, core) if core == which else (1 - group, far, side, core)

        return pairs(move)

    def shift(amount):
        return pairs(lambda group, far, side, core: (group, (far + amount) % lengths, side, core))

    return lengths, shift, axis_swap(0), axis_swap(1), pairs(lambda group, far, side, core: (group, far, side, 1 - core))


def dense_device(tokens, routes, placement, up_weight, down_weight, router_weight):
    groups, columns = lax.axis_size("dp"), lax.axis_size("expert")
    layers, tok_rows, _ = routes.shape
    model = tokens.shape[1]
    width = round_up(model + columns, LANES)
    lengths, shift, first_swap, second_swap, core_swap = dense_moves(groups, columns)
    axes = ("dp", "expert")
    ids = jnp.stack([lax.axis_index("expert"), lax.axis_index("dp")]).astype(jnp.int32)
    slots = jnp.arange(columns, dtype=jnp.int32)
    stream = tokens

    for layer in range(layers):
        chosen = routes[layer][:, :, None] == slots[None, None, :]
        target = jnp.sum(jnp.where(chosen, placement[layer][None, None, :], 0), axis=2)
        member = jnp.any(target[:, :, None] == slots[None, None, :], axis=1).astype(jnp.bfloat16)
        padding = jnp.zeros((tok_rows, width - model - columns), jnp.bfloat16)
        own = jnp.concatenate([rms_rows(stream), member, padding], axis=1)
        line = [own] + [lax.ppermute(own, axes, shift(step)) for step in range(1, lengths)]
        rows = jnp.concatenate(line, axis=0)
        rows = jnp.concatenate([rows, lax.ppermute(rows, axes, first_swap)], axis=0)
        near = jnp.concatenate([rows, lax.ppermute(rows, axes, second_swap)], axis=0)
        far = lax.ppermute(near, axes, core_swap)
        near_out, far_out = expert_ffn(layer, ids, near, far, router_weight, up_weight, down_weight)
        total = near_out.astype(jnp.float32) + lax.ppermute(far_out, axes, core_swap).astype(jnp.float32)
        for swap in (second_swap, first_swap):
            half = total.shape[0] // 2
            moved = lax.ppermute(total[half:].astype(jnp.bfloat16), axes, swap)
            total = total[:half] + moved.astype(jnp.float32)
        pieces = total.reshape(lengths, tok_rows, width)
        summed = pieces[0]
        for step in range(1, lengths):
            summed = summed + lax.ppermute(pieces[step].astype(jnp.bfloat16), axes, shift(lengths - step)).astype(jnp.float32)
        denominator = jnp.maximum(jnp.sum(summed[:, model:], axis=1, keepdims=True), 0.5)
        updated = stream.astype(jnp.float32) + summed[:, :model] / denominator
        stream = updated.astype(jnp.bfloat16)
    return stream


def slot_table(route_rows, place_row, columns, capacity):
    tok_rows, top_k = route_rows.shape
    experts = place_row.shape[0]
    matches = route_rows[:, :, None] == jnp.arange(experts, dtype=jnp.int32)[None, None, :]
    target = jnp.sum(jnp.where(matches, place_row[None, None, :], 0), axis=2).reshape(-1)
    row_count = target.shape[0]
    positions = jnp.arange(row_count, dtype=jnp.int32)
    earlier = (positions[None, :] < positions[:, None]) & (target[None, :] == target[:, None])
    row_rank = jnp.sum(earlier.astype(jnp.int32), axis=1)
    placed = (target[:, None, None] == jnp.arange(columns, dtype=jnp.int32)[None, :, None]) & (
        row_rank[:, None, None] == jnp.arange(capacity, dtype=jnp.int32)[None, None, :]
    )
    slot_map = jnp.sum(
        placed.reshape(tok_rows, top_k, columns, capacity).astype(jnp.float32), axis=1
    )
    return jnp.transpose(slot_map, (1, 2, 0))


def dispatch_device(tokens, routes, placement, up_weight, down_weight, router_weight):
    groups = lax.axis_size("dp")
    columns = lax.axis_size("expert")
    tok_rows = tokens.shape[0]
    top_k = routes.shape[2]
    capacity = 2 * tok_rows * top_k // columns

    def layer_step(stream, packed):
        route_rows, place_row, up_part, down_part, router_part = packed
        normed = rms_rows(stream)
        slot_map = slot_table(route_rows, place_row, columns, capacity)
        outgoing = jnp.einsum(
            "jct,td->jcd", slot_map.astype(jnp.bfloat16), normed, preferred_element_type=jnp.float32
        ).astype(jnp.bfloat16)
        arrived = lax.all_to_all(
            outgoing, "expert", split_axis=0, concat_axis=0, tiled=True
        ).reshape(columns * capacity, -1)
        affinity = jax.nn.sigmoid(
            jnp.dot(arrived, router_part[0], preferred_element_type=jnp.float32)
        ).astype(jnp.bfloat16)
        all_rows, all_gates = (
            lax.all_gather(arrived, "dp", axis=0, tiled=True),
            lax.all_gather(affinity, "dp", axis=0, tiled=True),
        )
        hidden = jax.nn.silu(
            jnp.dot(all_rows, up_part[0], preferred_element_type=jnp.float32)
        ).astype(jnp.bfloat16)
        part_sums = jnp.dot(hidden, down_part[0], preferred_element_type=jnp.float32).astype(
            jnp.bfloat16
        )
        part_sums = part_sums.reshape(groups, columns, capacity, -1)
        all_gates = all_gates.reshape(groups, columns, capacity)
        returned, gates_back = (
            lax.all_to_all(
                lax.all_to_all(part_sums, "dp", split_axis=0, concat_axis=0, tiled=True),
                "expert",
                split_axis=1,
                concat_axis=1,
                tiled=True,
            ),
            lax.all_to_all(
                lax.all_to_all(all_gates, "dp", split_axis=0, concat_axis=0, tiled=True),
                "expert",
                split_axis=1,
                concat_axis=1,
                tiled=True,
            ),
        )
        weights = slot_map * gates_back[0].astype(jnp.float32)[:, :, None]
        numerator = jnp.einsum(
            "ect,gecd->td",
            weights.astype(jnp.bfloat16),
            returned,
            preferred_element_type=jnp.float32,
        )
        denominator = jnp.sum(weights, axis=(0, 1))
        updated = stream.astype(jnp.float32) + numerator / jnp.maximum(denominator, 0.5)[:, None]
        return (updated.astype(jnp.bfloat16), None)

    result_stream, unused = lax.scan(
        layer_step, tokens, (routes, placement, up_weight, down_weight, router_weight)
    )
    return result_stream


def per_device(tokens, routes, placement, up_weight, down_weight, router_weight):
    groups, columns = lax.axis_size("dp"), lax.axis_size("expert")
    tok_rows, top_k = tokens.shape[0], routes.shape[2]
    capacity = 2 * tok_rows * top_k // columns
    dense = groups == 2 and columns % 4 == 0 and tok_rows <= 2 * capacity
    plan = dense_device if dense else dispatch_device
    return plan(tokens, routes, placement, up_weight, down_weight, router_weight)


def solution(mesh):
    return jax.shard_map(
        per_device,
        mesh=mesh,
        in_specs=(
            P(("dp", "expert"), None),
            P(None, ("dp", "expert"), None),
            P(),
            P(None, "expert", None, "dp"),
            P(None, "expert", "dp", None),
            P(None, "expert", None),
        ),
        out_specs=P(("dp", "expert"), None),
        check_vma=False,
    )
```

```python
import functools

import jax
import jax.numpy as jnp
from jax import lax
from jax.experimental import pallas as pl
from jax.experimental.pallas import tpu as pltpu
from jax.sharding import PartitionSpec as P

LANES = 128


def rms_rows(stream):
    values = stream.astype(jnp.float32)
    inverse = lax.rsqrt(jnp.mean(values * values, axis=-1, keepdims=True) + 1e-05)
    return (values * inverse).astype(jnp.bfloat16)


def round_up(value, unit):
    return -(-value // unit) * unit


VMEM = pl.BlockSpec(memory_space=pltpu.VMEM)
SMEM = pl.BlockSpec(memory_space=pltpu.SMEM)


def member_tail(layer, shift, lanes, routes_ref, placement_ref):
    top_k, tok_rows = routes_ref.shape[1:]
    experts = placement_ref.shape[1]
    ids = lax.broadcasted_iota(jnp.int32, (experts, tok_rows), 0)
    named = jnp.zeros((experts, tok_rows), jnp.float32)
    for choice in range(top_k):
        named = jnp.where(ids == routes_ref[layer, choice : choice + 1, :], 1.0, named)
    lane = lax.broadcasted_iota(jnp.int32, (lanes, experts), 0)
    served = jnp.where(lane == placement_ref[layer : layer + 1, :] + shift, 1.0, 0.0)
    return lax.dot_general(named, served, (((0,), (1,)), ((), ())), preferred_element_type=jnp.float32)


def write_payload(values, tail_rows, model, tail, payload_ref):
    inverse = lax.rsqrt(jnp.mean(values * values, axis=-1, keepdims=True) + 1e-05)
    normed = (values * inverse).astype(jnp.bfloat16)
    payload_ref[:, :tail] = normed[:, :tail]
    payload_ref[:, tail:] = tail_rows.astype(jnp.bfloat16)
    if model > tail:
        payload_ref[:, tail:model] = normed[:, tail:]


def first_kernel(model, tail, tokens_ref, routes_ref, placement_ref, payload_ref, tails_ref):
    lanes = payload_ref.shape[1] - tail
    for layer in range(routes_ref.shape[0]):
        tails_ref[layer] = member_tail(layer, model - tail, lanes, routes_ref, placement_ref)
    write_payload(tokens_ref[...].astype(jnp.float32), tails_ref[0], model, tail, payload_ref)


def update_kernel(model, tail, layer, last, own_ref, *refs):
    pieces, (stream_ref, tails_ref, updated_ref), more = refs[: len(refs) - 3 - (not last)], refs[len(refs) - 3 - (not last) :][:3], refs[len(refs) - (not last) :]
    total = own_ref[...]
    for piece in pieces:
        total = total + piece[...].astype(jnp.float32)
    denominator = jnp.maximum(jnp.sum(total[:, model:], axis=1, keepdims=True), 0.5)
    updated = (stream_ref[...].astype(jnp.float32) + total[:, :model] / denominator).astype(jnp.bfloat16)
    updated_ref[...] = updated
    if not last:
        write_payload(updated.astype(jnp.float32), tails_ref[layer + 1], model, tail, more[0])


def ffn_kernel(layer, near_ref, far_ref, router_ref, up_ref, down_ref, near_out, far_out, rows_ref, hidden_ref):
    half, width = near_ref.shape
    model, units = router_ref.shape[-1], up_ref.shape[2]
    rows_ref[:half, :] = near_ref[...]
    rows_ref[half:, :] = far_ref[...]
    slot, block = lax.axis_index("expert"), lax.axis_index("dp")
    tail = model // LANES * LANES
    lane = lax.broadcasted_iota(jnp.int32, (2 * half, width - tail), 1)
    here = lane == (model - tail) + slot
    member = jnp.sum(jnp.where(here, rows_ref[:, tail:].astype(jnp.float32), 0.0), axis=1, keepdims=True)
    by_rows = (((1,), (1,)), ((), ()))
    logits = lax.dot_general(rows_ref[:, :model], router_ref[...], by_rows, preferred_element_type=jnp.float32)
    gate = jax.nn.sigmoid(logits[:, layer : layer + 1]).astype(jnp.bfloat16).astype(jnp.float32) * member
    for start in range(0, units, 256):
        size = min(256, units - start)
        raw = lax.dot_general(
            rows_ref[:, :model], up_ref[layer, 0, start : start + size, :], by_rows, preferred_element_type=jnp.float32
        )
        hidden_ref[:, start : start + size] = jax.nn.silu(raw).astype(jnp.bfloat16)
    for start in range(0, model, 768):
        size = min(768, model - start)
        part = jnp.dot(hidden_ref[...], down_ref[layer, 0, :, start : start + size], preferred_element_type=jnp.float32)
        weighted = (part.astype(jnp.bfloat16).astype(jnp.float32) * gate).astype(jnp.bfloat16)
        near_out[:, start : start + size] = weighted[:half]
        far_out[:, start : start + size] = weighted[half:]
    sent = jnp.where(here & (block == 0), gate, 0.0)[:, model - tail :].astype(jnp.bfloat16)
    near_out[:, model:] = sent[:half]
    far_out[:, model:] = sent[half:]


def expert_ffn(layer, near, far, router, up, down):
    half, width = near.shape
    units = up.shape[2]
    return pl.pallas_call(
        functools.partial(ffn_kernel, layer),
        out_shape=[jax.ShapeDtypeStruct((half, width), jnp.bfloat16)] * 2,
        in_specs=[VMEM] * 5,
        out_specs=[VMEM] * 2,
        scratch_shapes=[pltpu.VMEM((2 * half, width), jnp.bfloat16), pltpu.VMEM((2 * half, units), jnp.bfloat16)],
        compiler_params=pltpu.CompilerParams(vmem_limit_bytes=16 * 1024 * 1024),
        name=f"ffn_{layer}",
    )(near, far, router, up, down)


def dense_moves(groups, columns):
    lengths = columns // 4

    def pairs(move):
        listed = []
        for group in range(groups):
            for far in range(lengths):
                for side in range(2):
                    for core in range(2):
                        to = move(group, far, side, core)
                        listed.append((((group * lengths + far) * 2 + side) * 2 + core, ((to[0] * lengths + to[1]) * 2 + to[2]) * 2 + to[3]))
        return listed

    def axis_swap(which):
        def move(group, far, side, core):
            return (group, far, 1 - side, core) if core == which else (1 - group, far, side, core)

        return pairs(move)

    def shift(amount):
        return pairs(lambda group, far, side, core: (group, (far + amount) % lengths, side, core))

    return lengths, shift, axis_swap(0), axis_swap(1), pairs(lambda group, far, side, core: (group, far, side, 1 - core))


def dense_device(tokens, routes, placement, up_weight, down_weight, router_weight):
    groups, columns = lax.axis_size("dp"), lax.axis_size("expert")
    layers, tok_rows, _ = routes.shape
    model = tokens.shape[1]
    width = round_up(model + columns, LANES)
    tail = model // LANES * LANES
    lengths, shift, first_swap, second_swap, core_swap = dense_moves(groups, columns)
    axes = ("dp", "expert")
    up_rows, router = jnp.swapaxes(up_weight, 2, 3), router_weight.reshape(layers, model)
    small = pltpu.CompilerParams(vmem_limit_bytes=4 * 1024 * 1024)
    payload_shape = jax.ShapeDtypeStruct((tok_rows, width), jnp.bfloat16)
    stream = tokens
    own, tails = pl.pallas_call(
        functools.partial(first_kernel, model, tail),
        out_shape=[payload_shape, jax.ShapeDtypeStruct((layers, tok_rows, width - tail), jnp.float32)],
        in_specs=[VMEM] * 3,
        out_specs=[VMEM] * 2,
        compiler_params=small,
        cost_estimate=pl.CostEstimate(flops=20_000_000_000, transcendentals=0, bytes_accessed=0),
        name="first",
    )(tokens, jnp.swapaxes(routes, 1, 2), placement)

    for layer in range(layers):
        line = [own] + [lax.ppermute(own, axes, shift(step)) for step in range(1, lengths)]
        rows = jnp.concatenate(line, axis=0)
        rows = jnp.concatenate([rows, lax.ppermute(rows, axes, first_swap)], axis=0)
        near = jnp.concatenate([rows, lax.ppermute(rows, axes, second_swap)], axis=0)
        far = lax.ppermute(near, axes, core_swap)
        near_out, far_out = expert_ffn(layer, near, far, router, up_rows, down_weight)
        total = near_out.astype(jnp.float32) + lax.ppermute(far_out, axes, core_swap).astype(jnp.float32)
        for swap in (second_swap, first_swap):
            half = total.shape[0] // 2
            moved = lax.ppermute(total[half:].astype(jnp.bfloat16), axes, swap)
            total = total[:half] + moved.astype(jnp.float32)
        pieces = total.reshape(lengths, tok_rows, width)
        arrived = [lax.ppermute(pieces[step].astype(jnp.bfloat16), axes, shift(lengths - step)) for step in range(1, lengths)]
        last = layer + 1 == layers
        outs = pl.pallas_call(
            functools.partial(update_kernel, model, tail, layer, last),
            out_shape=[jax.ShapeDtypeStruct(stream.shape, jnp.bfloat16)] + [payload_shape] * (not last),
            in_specs=[VMEM] * (len(arrived) + 3),
            out_specs=[VMEM] * (2 - last),
            compiler_params=small,
            name=f"update_{layer}",
        )(pieces[0], *arrived, stream, tails)
        stream, own = outs[0], outs[-1]
    return stream


def slot_table(route_rows, place_row, columns, capacity):
    tok_rows, top_k = route_rows.shape
    experts = place_row.shape[0]
    matches = route_rows[:, :, None] == jnp.arange(experts, dtype=jnp.int32)[None, None, :]
    target = jnp.sum(jnp.where(matches, place_row[None, None, :], 0), axis=2).reshape(-1)
    row_count = target.shape[0]
    positions = jnp.arange(row_count, dtype=jnp.int32)
    earlier = (positions[None, :] < positions[:, None]) & (target[None, :] == target[:, None])
    row_rank = jnp.sum(earlier.astype(jnp.int32), axis=1)
    placed = (target[:, None, None] == jnp.arange(columns, dtype=jnp.int32)[None, :, None]) & (
        row_rank[:, None, None] == jnp.arange(capacity, dtype=jnp.int32)[None, None, :]
    )
    slot_map = jnp.sum(
        placed.reshape(tok_rows, top_k, columns, capacity).astype(jnp.float32), axis=1
    )
    return jnp.transpose(slot_map, (1, 2, 0))


def dispatch_device(tokens, routes, placement, up_weight, down_weight, router_weight):
    groups = lax.axis_size("dp")
    columns = lax.axis_size("expert")
    tok_rows = tokens.shape[0]
    top_k = routes.shape[2]
    capacity = 2 * tok_rows * top_k // columns

    def layer_step(stream, packed):
        route_rows, place_row, up_part, down_part, router_part = packed
        normed = rms_rows(stream)
        slot_map = slot_table(route_rows, place_row, columns, capacity)
        outgoing = jnp.einsum(
            "jct,td->jcd", slot_map.astype(jnp.bfloat16), normed, preferred_element_type=jnp.float32
        ).astype(jnp.bfloat16)
        arrived = lax.all_to_all(
            outgoing, "expert", split_axis=0, concat_axis=0, tiled=True
        ).reshape(columns * capacity, -1)
        affinity = jax.nn.sigmoid(
            jnp.dot(arrived, router_part[0], preferred_element_type=jnp.float32)
        ).astype(jnp.bfloat16)
        all_rows, all_gates = (
            lax.all_gather(arrived, "dp", axis=0, tiled=True),
            lax.all_gather(affinity, "dp", axis=0, tiled=True),
        )
        hidden = jax.nn.silu(
            jnp.dot(all_rows, up_part[0], preferred_element_type=jnp.float32)
        ).astype(jnp.bfloat16)
        part_sums = jnp.dot(hidden, down_part[0], preferred_element_type=jnp.float32).astype(
            jnp.bfloat16
        )
        part_sums = part_sums.reshape(groups, columns, capacity, -1)
        all_gates = all_gates.reshape(groups, columns, capacity)
        returned, gates_back = (
            lax.all_to_all(
                lax.all_to_all(part_sums, "dp", split_axis=0, concat_axis=0, tiled=True),
                "expert",
                split_axis=1,
                concat_axis=1,
                tiled=True,
            ),
            lax.all_to_all(
                lax.all_to_all(all_gates, "dp", split_axis=0, concat_axis=0, tiled=True),
                "expert",
                split_axis=1,
                concat_axis=1,
                tiled=True,
            ),
        )
        weights = slot_map * gates_back[0].astype(jnp.float32)[:, :, None]
        numerator = jnp.einsum(
            "ect,gecd->td",
            weights.astype(jnp.bfloat16),
            returned,
            preferred_element_type=jnp.float32,
        )
        denominator = jnp.sum(weights, axis=(0, 1))
        updated = stream.astype(jnp.float32) + numerator / jnp.maximum(denominator, 0.5)[:, None]
        return (updated.astype(jnp.bfloat16), None)

    result_stream, unused = lax.scan(
        layer_step, tokens, (routes, placement, up_weight, down_weight, router_weight)
    )
    return result_stream


def per_device(tokens, routes, placement, up_weight, down_weight, router_weight):
    groups, columns = lax.axis_size("dp"), lax.axis_size("expert")
    tok_rows, top_k = tokens.shape[0], routes.shape[2]
    capacity = 2 * tok_rows * top_k // columns
    dense = groups == 2 and columns % 4 == 0 and tok_rows <= 2 * capacity
    plan = dense_device if dense else dispatch_device
    return plan(tokens, routes, placement, up_weight, down_weight, router_weight)


def solution(mesh):
    return jax.shard_map(
        per_device,
        mesh=mesh,
        in_specs=(
            P(("dp", "expert"), None),
            P(None, ("dp", "expert"), None),
            P(),
            P(None, "expert", None, "dp"),
            P(None, "expert", "dp", None),
            P(None, "expert", None),
        ),
        out_specs=P(("dp", "expert"), None),
        check_vma=False,
    )
```

```python
import functools

import jax
import jax.numpy as jnp
from jax import lax
from jax.experimental import pallas as pl
from jax.experimental.pallas import tpu as pltpu
from jax.sharding import PartitionSpec as P

LANES = 128


def rms_rows(stream):
    values = stream.astype(jnp.float32)
    inverse = lax.rsqrt(jnp.mean(values * values, axis=-1, keepdims=True) + 1e-05)
    return (values * inverse).astype(jnp.bfloat16)


def round_up(value, unit):
    return -(-value // unit) * unit


VMEM = pl.BlockSpec(memory_space=pltpu.VMEM)
SMEM = pl.BlockSpec(memory_space=pltpu.SMEM)


def member_tail(layer, shift, lanes, routes_ref, placement_ref):
    top_k, tok_rows = routes_ref.shape[1:]
    experts = placement_ref.shape[1]
    ids = lax.broadcasted_iota(jnp.int32, (experts, tok_rows), 0)
    named = jnp.zeros((experts, tok_rows), jnp.float32)
    for choice in range(top_k):
        named = jnp.where(ids == routes_ref[layer, choice : choice + 1, :], 1.0, named)
    lane = lax.broadcasted_iota(jnp.int32, (lanes, experts), 0)
    served = jnp.where(lane == placement_ref[layer : layer + 1, :] + shift, 1.0, 0.0)
    return lax.dot_general(named, served, (((0,), (1,)), ((), ())), preferred_element_type=jnp.float32)


def write_payload(values, tail_rows, model, tail, payload_ref):
    inverse = lax.rsqrt(jnp.mean(values * values, axis=-1, keepdims=True) + 1e-05)
    normed = (values * inverse).astype(jnp.bfloat16)
    payload_ref[:, :tail] = normed[:, :tail]
    payload_ref[:, tail:] = tail_rows.astype(jnp.bfloat16)
    if model > tail:
        payload_ref[:, tail:model] = normed[:, tail:]


def first_kernel(model, tail, tokens_ref, routes_ref, placement_ref, payload_ref, tails_ref):
    lanes = payload_ref.shape[1] - tail
    for layer in range(routes_ref.shape[0]):
        tails_ref[layer] = member_tail(layer, model - tail, lanes, routes_ref, placement_ref)
    write_payload(tokens_ref[...].astype(jnp.float32), tails_ref[0], model, tail, payload_ref)


def update_kernel(model, tail, layer, last, own_ref, *refs):
    pieces, (stream_ref, tails_ref, updated_ref), more = refs[: len(refs) - 3 - (not last)], refs[len(refs) - 3 - (not last) :][:3], refs[len(refs) - (not last) :]
    total = own_ref[...]
    for piece in pieces:
        total = total + piece[...].astype(jnp.float32)
    denominator = jnp.maximum(jnp.sum(total[:, model:], axis=1, keepdims=True), 0.5)
    updated = (stream_ref[...].astype(jnp.float32) + total[:, :model] / denominator).astype(jnp.bfloat16)
    updated_ref[...] = updated
    if not last:
        write_payload(updated.astype(jnp.float32), tails_ref[layer + 1], model, tail, more[0])


def ffn_kernel(layer, count, *refs):
    pieces, (router_ref, up_ref, down_ref), outs, (rows_ref, hidden_ref) = refs[:count], refs[count : count + 3], refs[count + 3 : -2], refs[-2:]
    size, width = pieces[0].shape
    model, units = router_ref.shape[-1], up_ref.shape[2]
    for index, piece in enumerate(pieces):
        rows_ref[index * size : (index + 1) * size, :] = piece[...]
    slot, block = lax.axis_index("expert"), lax.axis_index("dp")
    tail = model // LANES * LANES
    lane = lax.broadcasted_iota(jnp.int32, (count * size, width - tail), 1)
    here = lane == (model - tail) + slot
    member = jnp.sum(jnp.where(here, rows_ref[:, tail:].astype(jnp.float32), 0.0), axis=1, keepdims=True)
    by_rows = (((1,), (1,)), ((), ()))
    logits = lax.dot_general(rows_ref[:, :model], router_ref[...], by_rows, preferred_element_type=jnp.float32)
    gate = jax.nn.sigmoid(logits[:, layer : layer + 1]).astype(jnp.bfloat16).astype(jnp.float32) * member
    for start in range(0, units, 256):
        stop = min(start + 256, units)
        raw = lax.dot_general(rows_ref[:, :model], up_ref[layer, 0, start:stop, :], by_rows, preferred_element_type=jnp.float32)
        hidden_ref[:, start:stop] = jax.nn.silu(raw).astype(jnp.bfloat16)
    for start in range(0, model, 768):
        stop = min(start + 768, model)
        part = jnp.dot(hidden_ref[...], down_ref[layer, 0, :, start:stop], preferred_element_type=jnp.float32)
        weighted = (part.astype(jnp.bfloat16).astype(jnp.float32) * gate).astype(jnp.bfloat16)
        for index, out in enumerate(outs):
            out[:, start:stop] = weighted[index * size : (index + 1) * size]
    sent = jnp.where(here & (block == 0), gate, 0.0)[:, model - tail :].astype(jnp.bfloat16)
    for index, out in enumerate(outs):
        out[:, model:] = sent[index * size : (index + 1) * size]


def expert_ffn(layer, pieces, router, up, down):
    count, (size, width), units = len(pieces), pieces[0].shape, up.shape[2]
    return pl.pallas_call(
        functools.partial(ffn_kernel, layer, count),
        out_shape=[jax.ShapeDtypeStruct((size, width), jnp.bfloat16)] * count,
        in_specs=[VMEM] * (count + 3),
        out_specs=[VMEM] * count,
        scratch_shapes=[pltpu.VMEM((count * size, width), jnp.bfloat16), pltpu.VMEM((count * size, units), jnp.bfloat16)],
        compiler_params=pltpu.CompilerParams(vmem_limit_bytes=16 * 1024 * 1024),
        name=f"ffn_{layer}",
    )(*pieces, router, up, down)


def dense_moves(groups, columns):
    lengths = columns // 4

    def pairs(move):
        listed = []
        for group in range(groups):
            for far in range(lengths):
                for side in range(2):
                    for core in range(2):
                        to = move(group, far, side, core)
                        listed.append((((group * lengths + far) * 2 + side) * 2 + core, ((to[0] * lengths + to[1]) * 2 + to[2]) * 2 + to[3]))
        return listed

    def axis_swap(which):
        def move(group, far, side, core):
            return (group, far, 1 - side, core) if core == which else (1 - group, far, side, core)

        return pairs(move)

    def shift(amount):
        return pairs(lambda group, far, side, core: (group, far ^ amount, side, core))

    return lengths, shift, axis_swap(0), axis_swap(1), pairs(lambda group, far, side, core: (group, far, side, 1 - core))


def dense_device(tokens, routes, placement, up_weight, down_weight, router_weight):
    groups, columns = lax.axis_size("dp"), lax.axis_size("expert")
    layers, tok_rows, _ = routes.shape
    model = tokens.shape[1]
    width = round_up(model + columns, LANES)
    tail = model // LANES * LANES
    lengths, shift, first_swap, second_swap, core_swap = dense_moves(groups, columns)
    axes = ("dp", "expert")
    up_rows, router = jnp.swapaxes(up_weight, 2, 3), router_weight.reshape(layers, model)
    small = pltpu.CompilerParams(vmem_limit_bytes=4 * 1024 * 1024)
    payload_shape = jax.ShapeDtypeStruct((tok_rows, width), jnp.bfloat16)
    stream = tokens
    own, tails = pl.pallas_call(
        functools.partial(first_kernel, model, tail),
        out_shape=[payload_shape, jax.ShapeDtypeStruct((layers, tok_rows, width - tail), jnp.float32)],
        in_specs=[VMEM] * 3,
        out_specs=[VMEM] * 2,
        compiler_params=small,
        cost_estimate=pl.CostEstimate(flops=20_000_000_000, transcendentals=0, bytes_accessed=0),
        name="first",
    )(tokens, jnp.swapaxes(routes, 1, 2), placement)

    def move(value, pairs):
        return lax.ppermute(value, axes, pairs)

    for layer in range(layers):
        here = jnp.concatenate([own] + [move(own, shift(step)) for step in range(1, lengths)], axis=0)
        first = move(here, first_swap)
        second = move(here, second_swap)
        across = move(first, second_swap)
        near = [here, second, first, across]
        outs = expert_ffn(layer, near + [move(piece, core_swap) for piece in near], router, up_rows, down_weight)
        wide = [value.astype(jnp.float32) for value in outs[:4]]
        here, second, first, across = [
            mine + move(theirs, core_swap).astype(jnp.float32) for mine, theirs in zip(wide, outs[4:])
        ]
        first = first + move(across.astype(jnp.bfloat16), second_swap).astype(jnp.float32)
        here = here + move(second.astype(jnp.bfloat16), second_swap).astype(jnp.float32)
        here = here + move(first.astype(jnp.bfloat16), first_swap).astype(jnp.float32)
        pieces = here.reshape(lengths, tok_rows, width)
        arrived = [move(pieces[step].astype(jnp.bfloat16), shift(step)) for step in range(1, lengths)]
        last = layer + 1 == layers
        outs = pl.pallas_call(
            functools.partial(update_kernel, model, tail, layer, last),
            out_shape=[jax.ShapeDtypeStruct(stream.shape, jnp.bfloat16)] + [payload_shape] * (not last),
            in_specs=[VMEM] * (len(arrived) + 3),
            out_specs=[VMEM] * (2 - last),
            compiler_params=small,
            name=f"update_{layer}",
        )(pieces[0], *arrived, stream, tails)
        stream, own = outs[0], outs[-1]
    return stream


def slot_table(route_rows, place_row, columns, capacity):
    tok_rows, top_k = route_rows.shape
    experts = place_row.shape[0]
    matches = route_rows[:, :, None] == jnp.arange(experts, dtype=jnp.int32)[None, None, :]
    target = jnp.sum(jnp.where(matches, place_row[None, None, :], 0), axis=2).reshape(-1)
    row_count = target.shape[0]
    positions = jnp.arange(row_count, dtype=jnp.int32)
    earlier = (positions[None, :] < positions[:, None]) & (target[None, :] == target[:, None])
    row_rank = jnp.sum(earlier.astype(jnp.int32), axis=1)
    placed = (target[:, None, None] == jnp.arange(columns, dtype=jnp.int32)[None, :, None]) & (
        row_rank[:, None, None] == jnp.arange(capacity, dtype=jnp.int32)[None, None, :]
    )
    slot_map = jnp.sum(
        placed.reshape(tok_rows, top_k, columns, capacity).astype(jnp.float32), axis=1
    )
    return jnp.transpose(slot_map, (1, 2, 0))


def dispatch_device(tokens, routes, placement, up_weight, down_weight, router_weight):
    groups = lax.axis_size("dp")
    columns = lax.axis_size("expert")
    tok_rows = tokens.shape[0]
    top_k = routes.shape[2]
    capacity = 2 * tok_rows * top_k // columns

    def layer_step(stream, packed):
        route_rows, place_row, up_part, down_part, router_part = packed
        normed = rms_rows(stream)
        slot_map = slot_table(route_rows, place_row, columns, capacity)
        outgoing = jnp.einsum(
            "jct,td->jcd", slot_map.astype(jnp.bfloat16), normed, preferred_element_type=jnp.float32
        ).astype(jnp.bfloat16)
        arrived = lax.all_to_all(
            outgoing, "expert", split_axis=0, concat_axis=0, tiled=True
        ).reshape(columns * capacity, -1)
        affinity = jax.nn.sigmoid(
            jnp.dot(arrived, router_part[0], preferred_element_type=jnp.float32)
        ).astype(jnp.bfloat16)
        all_rows, all_gates = (
            lax.all_gather(arrived, "dp", axis=0, tiled=True),
            lax.all_gather(affinity, "dp", axis=0, tiled=True),
        )
        hidden = jax.nn.silu(
            jnp.dot(all_rows, up_part[0], preferred_element_type=jnp.float32)
        ).astype(jnp.bfloat16)
        part_sums = jnp.dot(hidden, down_part[0], preferred_element_type=jnp.float32).astype(
            jnp.bfloat16
        )
        part_sums = part_sums.reshape(groups, columns, capacity, -1)
        all_gates = all_gates.reshape(groups, columns, capacity)
        returned, gates_back = (
            lax.all_to_all(
                lax.all_to_all(part_sums, "dp", split_axis=0, concat_axis=0, tiled=True),
                "expert",
                split_axis=1,
                concat_axis=1,
                tiled=True,
            ),
            lax.all_to_all(
                lax.all_to_all(all_gates, "dp", split_axis=0, concat_axis=0, tiled=True),
                "expert",
                split_axis=1,
                concat_axis=1,
                tiled=True,
            ),
        )
        weights = slot_map * gates_back[0].astype(jnp.float32)[:, :, None]
        numerator = jnp.einsum(
            "ect,gecd->td",
            weights.astype(jnp.bfloat16),
            returned,
            preferred_element_type=jnp.float32,
        )
        denominator = jnp.sum(weights, axis=(0, 1))
        updated = stream.astype(jnp.float32) + numerator / jnp.maximum(denominator, 0.5)[:, None]
        return (updated.astype(jnp.bfloat16), None)

    result_stream, unused = lax.scan(
        layer_step, tokens, (routes, placement, up_weight, down_weight, router_weight)
    )
    return result_stream


def per_device(tokens, routes, placement, up_weight, down_weight, router_weight):
    groups, columns = lax.axis_size("dp"), lax.axis_size("expert")
    tok_rows, top_k = tokens.shape[0], routes.shape[2]
    capacity = 2 * tok_rows * top_k // columns
    lengths = columns // 4
    dense = groups == 2 and columns == 4 * lengths and lengths & (lengths - 1) == 0 and tok_rows <= 2 * capacity
    plan = dense_device if dense else dispatch_device
    return plan(tokens, routes, placement, up_weight, down_weight, router_weight)


def solution(mesh):
    return jax.shard_map(
        per_device,
        mesh=mesh,
        in_specs=(
            P(("dp", "expert"), None),
            P(None, ("dp", "expert"), None),
            P(),
            P(None, "expert", None, "dp"),
            P(None, "expert", "dp", None),
            P(None, "expert", None),
        ),
        out_specs=P(("dp", "expert"), None),
        check_vma=False,
    )
```

```python
import functools

import jax
import jax.numpy as jnp
from jax import lax
from jax.experimental import pallas as pl
from jax.experimental.pallas import tpu as pltpu
from jax.sharding import PartitionSpec as P

LANES = 128
WAVES = 2


def rms_rows(stream):
    values = stream.astype(jnp.float32)
    inverse = lax.rsqrt(jnp.mean(values * values, axis=-1, keepdims=True) + 1e-05)
    return (values * inverse).astype(jnp.bfloat16)


def round_up(value, unit):
    return -(-value // unit) * unit


VMEM = pl.BlockSpec(memory_space=pltpu.VMEM)
SMEM = pl.BlockSpec(memory_space=pltpu.SMEM)


def member_tail(layer, shift, lanes, tok_rows, experts, table_ref):
    top_k = table_ref.shape[1] - 1
    ids = lax.broadcasted_iota(jnp.int32, (experts, tok_rows), 0)
    named = jnp.zeros((experts, tok_rows), jnp.float32)
    for choice in range(top_k):
        named = jnp.where(ids == table_ref[layer, choice : choice + 1, :tok_rows], 1.0, named)
    lane = lax.broadcasted_iota(jnp.int32, (lanes, experts), 0)
    served = jnp.where(lane == table_ref[layer, top_k : top_k + 1, :experts] + shift, 1.0, 0.0)
    return lax.dot_general(named, served, (((0,), (1,)), ((), ())), preferred_element_type=jnp.float32)


def write_payload(values, tail_rows, model, tail, payload_ref):
    inverse = lax.rsqrt(jnp.mean(values * values, axis=-1, keepdims=True) + 1e-05)
    normed = (values * inverse).astype(jnp.bfloat16)
    payload_ref[:, :tail] = normed[:, :tail]
    payload_ref[:, tail:] = tail_rows.astype(jnp.bfloat16)
    if model > tail:
        payload_ref[:, tail:model] = normed[:, tail:]


def first_kernel(model, tail, experts, tokens_ref, table_ref, payload_ref, tails_ref):
    lanes = payload_ref.shape[1] - tail
    for layer in range(table_ref.shape[0]):
        tails_ref[layer] = member_tail(layer, model - tail, lanes, tokens_ref.shape[0], experts, table_ref)
    write_payload(tokens_ref[...].astype(jnp.float32), tails_ref[0], model, tail, payload_ref)


def update_kernel(model, tail, layer, last, own_ref, *refs):
    pieces, (stream_ref, tails_ref, updated_ref), more = refs[: len(refs) - 3 - (not last)], refs[len(refs) - 3 - (not last) :][:3], refs[len(refs) - (not last) :]
    total = own_ref[...]
    for piece in pieces:
        total = total + piece[...].astype(jnp.float32)
    denominator = jnp.maximum(jnp.sum(total[:, model:], axis=1, keepdims=True), 0.5)
    updated = (stream_ref[...].astype(jnp.float32) + total[:, :model] / denominator).astype(jnp.bfloat16)
    updated_ref[...] = updated
    if not last:
        write_payload(updated.astype(jnp.float32), tails_ref[layer + 1], model, tail, more[0])


def ffn_kernel(layer, count, *refs):
    pieces, (router_ref, up_ref, down_ref), outs, (rows_ref, hidden_ref) = refs[:count], refs[count : count + 3], refs[count + 3 : -2], refs[-2:]
    total, width = rows_ref.shape
    model, units = router_ref.shape[-1], up_ref.shape[2]
    size, filled = outs[0].shape[0], 0
    for piece in pieces:
        rows_ref[filled : filled + piece.shape[0], :] = piece[...]
        filled += piece.shape[0]
    slot, block = lax.axis_index("expert"), lax.axis_index("dp")
    tail = model // LANES * LANES
    lane = lax.broadcasted_iota(jnp.int32, (total, width - tail), 1)
    here = lane == (model - tail) + slot
    member = jnp.sum(jnp.where(here, rows_ref[:, tail:].astype(jnp.float32), 0.0), axis=1, keepdims=True)
    by_rows = (((1,), (1,)), ((), ()))
    logits = lax.dot_general(rows_ref[:, :model], router_ref[...], by_rows, preferred_element_type=jnp.float32)
    gate = jax.nn.sigmoid(logits[:, layer : layer + 1]).astype(jnp.bfloat16).astype(jnp.float32) * member
    for start in range(0, units, 256):
        stop = min(start + 256, units)
        raw = lax.dot_general(rows_ref[:, :model], up_ref[layer, 0, start:stop, :], by_rows, preferred_element_type=jnp.float32)
        hidden_ref[:, start:stop] = jax.nn.silu(raw).astype(jnp.bfloat16)
    for start in range(0, model, 768):
        stop = min(start + 768, model)
        part = jnp.dot(hidden_ref[...], down_ref[layer, 0, :, start:stop], preferred_element_type=jnp.float32)
        weighted = (part.astype(jnp.bfloat16).astype(jnp.float32) * gate).astype(jnp.bfloat16)
        for index, out in enumerate(outs):
            out[:, start:stop] = weighted[index * size : (index + 1) * size]
    sent = jnp.where(here & (block == 0), gate, 0.0)[:, model - tail :].astype(jnp.bfloat16)
    for index, out in enumerate(outs):
        out[:, model:] = sent[index * size : (index + 1) * size]


def expert_ffn(layer, pieces, router, up, down):
    count, width, units = len(pieces), pieces[0].shape[1], up.shape[2]
    total = sum(piece.shape[0] for piece in pieces)
    return pl.pallas_call(
        functools.partial(ffn_kernel, layer, count),
        out_shape=[jax.ShapeDtypeStruct((total // 8, width), jnp.bfloat16)] * 8,
        in_specs=[VMEM] * (count + 3),
        out_specs=[VMEM] * 8,
        scratch_shapes=[pltpu.VMEM((total, width), jnp.bfloat16), pltpu.VMEM((total, units), jnp.bfloat16)],
        compiler_params=pltpu.CompilerParams(vmem_limit_bytes=16 * 1024 * 1024),
        name=f"ffn_{layer}",
    )(*pieces, router, up, down)


def dense_moves(groups, columns):
    lengths = columns // 4

    def pairs(move):
        listed = []
        for group in range(groups):
            for far in range(lengths):
                for side in range(2):
                    for core in range(2):
                        to = move(group, far, side, core)
                        listed.append((((group * lengths + far) * 2 + side) * 2 + core, ((to[0] * lengths + to[1]) * 2 + to[2]) * 2 + to[3]))
        return listed

    def axis_swap(which):
        def move(group, far, side, core):
            return (group, far, 1 - side, core) if core == which else (1 - group, far, side, core)

        return pairs(move)

    def shift(amount):
        return pairs(lambda group, far, side, core: (group, far ^ amount, side, core))

    return lengths, shift, axis_swap(0), axis_swap(1), pairs(lambda group, far, side, core: (group, far, side, 1 - core))


def dense_device(tokens, routes, placement, up_weight, down_weight, router_weight):
    groups, columns = lax.axis_size("dp"), lax.axis_size("expert")
    layers, tok_rows, _ = routes.shape
    model = tokens.shape[1]
    width = round_up(model + columns, LANES)
    tail = model // LANES * LANES
    lengths, shift, first_swap, second_swap, core_swap = dense_moves(groups, columns)
    axes = ("dp", "expert")
    up_rows, router = jnp.swapaxes(up_weight, 2, 3), router_weight.reshape(layers, model)
    small = pltpu.CompilerParams(vmem_limit_bytes=4 * 1024 * 1024)
    payload_shape = jax.ShapeDtypeStruct((tok_rows, width), jnp.bfloat16)
    top_k, experts = routes.shape[2], placement.shape[1]
    lanes = max(tok_rows, experts)
    table = lax.pad(jnp.swapaxes(routes, 1, 2), 0, [(0, 0, 0), (0, 1, 0), (0, lanes - tok_rows, 0)]) + lax.pad(
        placement[:, None, :], 0, [(0, 0, 0), (top_k, 0, 0), (0, lanes - experts, 0)]
    )
    stream = tokens
    own, tails = pl.pallas_call(
        functools.partial(first_kernel, model, tail, experts),
        out_shape=[payload_shape, jax.ShapeDtypeStruct((layers, tok_rows, width - tail), jnp.float32)],
        in_specs=[VMEM] * 2,
        out_specs=[VMEM] * 2,
        compiler_params=small,
        cost_estimate=pl.CostEstimate(flops=20_000_000_000, transcendentals=0, bytes_accessed=0),
        name="first",
    )(tokens, table)

    wave = lengths // WAVES

    def move(value, pairs):
        return lax.ppermute(value, axes, pairs)

    for layer in range(layers):
        line = [own] + [move(own, shift(step)) for step in range(1, lengths)]
        parts = [jnp.concatenate(line[start : start + wave], axis=0) for start in range(0, lengths, wave)]
        here = jnp.concatenate(line, axis=0)
        firsts = [move(part, first_swap) for part in parts]
        second = move(here, second_swap)
        acrosses = [move(part, second_swap) for part in firsts]
        near = [here, second] + firsts + acrosses
        outs = expert_ffn(layer, near + [move(piece, core_swap) for piece in near], router, up_rows, down_weight)
        here, second, first, across = [
            mine.astype(jnp.float32) + move(theirs, core_swap).astype(jnp.float32) for mine, theirs in zip(outs[:4], outs[4:])
        ]
        first = first + move(across.astype(jnp.bfloat16), second_swap).astype(jnp.float32)
        here = here + move(second.astype(jnp.bfloat16), second_swap).astype(jnp.float32)
        here = here + move(first.astype(jnp.bfloat16), first_swap).astype(jnp.float32)
        pieces = here.reshape(lengths, tok_rows, width)
        arrived = [move(pieces[step].astype(jnp.bfloat16), shift(step)) for step in range(1, lengths)]
        last = layer + 1 == layers
        outs = pl.pallas_call(
            functools.partial(update_kernel, model, tail, layer, last),
            out_shape=[jax.ShapeDtypeStruct(stream.shape, jnp.bfloat16)] + [payload_shape] * (not last),
            in_specs=[VMEM] * (len(arrived) + 3),
            out_specs=[VMEM] * (2 - last),
            compiler_params=small,
            name=f"update_{layer}",
        )(pieces[0], *arrived, stream, tails)
        stream, own = outs[0], outs[-1]
    return stream


def slot_table(route_rows, place_row, columns, capacity):
    tok_rows, top_k = route_rows.shape
    experts = place_row.shape[0]
    matches = route_rows[:, :, None] == jnp.arange(experts, dtype=jnp.int32)[None, None, :]
    target = jnp.sum(jnp.where(matches, place_row[None, None, :], 0), axis=2).reshape(-1)
    row_count = target.shape[0]
    positions = jnp.arange(row_count, dtype=jnp.int32)
    earlier = (positions[None, :] < positions[:, None]) & (target[None, :] == target[:, None])
    row_rank = jnp.sum(earlier.astype(jnp.int32), axis=1)
    placed = (target[:, None, None] == jnp.arange(columns, dtype=jnp.int32)[None, :, None]) & (
        row_rank[:, None, None] == jnp.arange(capacity, dtype=jnp.int32)[None, None, :]
    )
    slot_map = jnp.sum(
        placed.reshape(tok_rows, top_k, columns, capacity).astype(jnp.float32), axis=1
    )
    return jnp.transpose(slot_map, (1, 2, 0))


def dispatch_device(tokens, routes, placement, up_weight, down_weight, router_weight):
    groups = lax.axis_size("dp")
    columns = lax.axis_size("expert")
    tok_rows = tokens.shape[0]
    top_k = routes.shape[2]
    capacity = 2 * tok_rows * top_k // columns

    def layer_step(stream, packed):
        route_rows, place_row, up_part, down_part, router_part = packed
        normed = rms_rows(stream)
        slot_map = slot_table(route_rows, place_row, columns, capacity)
        outgoing = jnp.einsum(
            "jct,td->jcd", slot_map.astype(jnp.bfloat16), normed, preferred_element_type=jnp.float32
        ).astype(jnp.bfloat16)
        arrived = lax.all_to_all(
            outgoing, "expert", split_axis=0, concat_axis=0, tiled=True
        ).reshape(columns * capacity, -1)
        affinity = jax.nn.sigmoid(
            jnp.dot(arrived, router_part[0], preferred_element_type=jnp.float32)
        ).astype(jnp.bfloat16)
        all_rows, all_gates = (
            lax.all_gather(arrived, "dp", axis=0, tiled=True),
            lax.all_gather(affinity, "dp", axis=0, tiled=True),
        )
        hidden = jax.nn.silu(
            jnp.dot(all_rows, up_part[0], preferred_element_type=jnp.float32)
        ).astype(jnp.bfloat16)
        part_sums = jnp.dot(hidden, down_part[0], preferred_element_type=jnp.float32).astype(
            jnp.bfloat16
        )
        part_sums = part_sums.reshape(groups, columns, capacity, -1)
        all_gates = all_gates.reshape(groups, columns, capacity)
        returned, gates_back = (
            lax.all_to_all(
                lax.all_to_all(part_sums, "dp", split_axis=0, concat_axis=0, tiled=True),
                "expert",
                split_axis=1,
                concat_axis=1,
                tiled=True,
            ),
            lax.all_to_all(
                lax.all_to_all(all_gates, "dp", split_axis=0, concat_axis=0, tiled=True),
                "expert",
                split_axis=1,
                concat_axis=1,
                tiled=True,
            ),
        )
        weights = slot_map * gates_back[0].astype(jnp.float32)[:, :, None]
        numerator = jnp.einsum(
            "ect,gecd->td",
            weights.astype(jnp.bfloat16),
            returned,
            preferred_element_type=jnp.float32,
        )
        denominator = jnp.sum(weights, axis=(0, 1))
        updated = stream.astype(jnp.float32) + numerator / jnp.maximum(denominator, 0.5)[:, None]
        return (updated.astype(jnp.bfloat16), None)

    result_stream, unused = lax.scan(
        layer_step, tokens, (routes, placement, up_weight, down_weight, router_weight)
    )
    return result_stream


def per_device(tokens, routes, placement, up_weight, down_weight, router_weight):
    groups, columns = lax.axis_size("dp"), lax.axis_size("expert")
    tok_rows, top_k = tokens.shape[0], routes.shape[2]
    capacity = 2 * tok_rows * top_k // columns
    lengths = columns // 4
    dense = groups == 2 and columns == 4 * lengths and lengths & (lengths - 1) == 0 and tok_rows <= 2 * capacity
    plan = dense_device if dense else dispatch_device
    return plan(tokens, routes, placement, up_weight, down_weight, router_weight)


def solution(mesh):
    return jax.shard_map(
        per_device,
        mesh=mesh,
        in_specs=(
            P(("dp", "expert"), None),
            P(None, ("dp", "expert"), None),
            P(),
            P(None, "expert", None, "dp"),
            P(None, "expert", "dp", None),
            P(None, "expert", None),
        ),
        out_specs=P(("dp", "expert"), None),
        check_vma=False,
    )
```

```python
import functools

import jax
import jax.numpy as jnp
from jax import lax
from jax.experimental import pallas as pl
from jax.experimental.pallas import tpu as pltpu
from jax.sharding import PartitionSpec as P

LANES = 128
WAVES = 2


def rms_rows(stream):
    values = stream.astype(jnp.float32)
    inverse = lax.rsqrt(jnp.mean(values * values, axis=-1, keepdims=True) + 1e-05)
    return (values * inverse).astype(jnp.bfloat16)


def round_up(value, unit):
    return -(-value // unit) * unit


VMEM = pl.BlockSpec(memory_space=pltpu.VMEM)
SMEM = pl.BlockSpec(memory_space=pltpu.SMEM)


def member_tail(layer, shift, lanes, tok_rows, experts, table_ref):
    top_k = table_ref.shape[1] - 1
    ids = lax.broadcasted_iota(jnp.int32, (experts, tok_rows), 0)
    named = jnp.zeros((experts, tok_rows), jnp.float32)
    for choice in range(top_k):
        named = jnp.where(ids == table_ref[layer, choice : choice + 1, :tok_rows], 1.0, named)
    lane = lax.broadcasted_iota(jnp.int32, (lanes, experts), 0)
    served = jnp.where(lane == table_ref[layer, top_k : top_k + 1, :experts] + shift, 1.0, 0.0)
    return lax.dot_general(named, served, (((0,), (1,)), ((), ())), preferred_element_type=jnp.float32)


def write_payload(values, tail_rows, model, tail, payload_ref):
    inverse = lax.rsqrt(jnp.mean(values * values, axis=-1, keepdims=True) + 1e-05)
    normed = (values * inverse).astype(jnp.bfloat16)
    payload_ref[:, :tail] = normed[:, :tail]
    payload_ref[:, tail:] = tail_rows.astype(jnp.bfloat16)
    if model > tail:
        payload_ref[:, tail:model] = normed[:, tail:]


def first_kernel(model, tail, experts, tokens_ref, table_ref, payload_ref, tails_ref):
    lanes = payload_ref.shape[1] - tail
    for layer in range(table_ref.shape[0]):
        tails_ref[layer] = member_tail(layer, model - tail, lanes, tokens_ref.shape[0], experts, table_ref)
    write_payload(tokens_ref[...].astype(jnp.float32), tails_ref[0], model, tail, payload_ref)


def update_kernel(model, tail, layer, last, own_ref, *refs):
    pieces, (stream_ref, tails_ref, updated_ref), more = refs[: len(refs) - 3 - (not last)], refs[len(refs) - 3 - (not last) :][:3], refs[len(refs) - (not last) :]
    total = own_ref[...]
    for piece in pieces:
        total = total + piece[...].astype(jnp.float32)
    denominator = jnp.maximum(jnp.sum(total[:, model:], axis=1, keepdims=True), 0.5)
    updated = (stream_ref[...].astype(jnp.float32) + total[:, :model] / denominator).astype(jnp.bfloat16)
    updated_ref[...] = updated
    if not last:
        write_payload(updated.astype(jnp.float32), tails_ref[layer + 1], model, tail, more[0])


def ffn_kernel(layer, count, *refs):
    pieces, (router_ref, up_ref, down_ref), outs, (rows_ref, hidden_ref) = refs[:count], refs[count : count + 3], refs[count + 3 : -2], refs[-2:]
    total, width = rows_ref.shape
    model, units = router_ref.shape[-1], up_ref.shape[2]
    size, filled = outs[0].shape[0], 0
    for piece in pieces:
        rows_ref[filled : filled + piece.shape[0], :] = piece[...]
        filled += piece.shape[0]
    slot, block = lax.axis_index("expert"), lax.axis_index("dp")
    tail = model // LANES * LANES
    lane = lax.broadcasted_iota(jnp.int32, (total, width - tail), 1)
    here = lane == (model - tail) + slot
    member = jnp.sum(jnp.where(here, rows_ref[:, tail:].astype(jnp.float32), 0.0), axis=1, keepdims=True)
    by_rows = (((1,), (1,)), ((), ()))
    logits = lax.dot_general(rows_ref[:, :model], router_ref[...], by_rows, preferred_element_type=jnp.float32)
    gate = jax.nn.sigmoid(logits[:, layer : layer + 1]).astype(jnp.bfloat16).astype(jnp.float32) * member
    for start in range(0, units, 256):
        stop = min(start + 256, units)
        raw = lax.dot_general(rows_ref[:, :model], up_ref[layer, 0, start:stop, :], by_rows, preferred_element_type=jnp.float32)
        hidden_ref[:, start:stop] = jax.nn.silu(raw).astype(jnp.bfloat16)
    for start in range(0, model, 768):
        stop = min(start + 768, model)
        part = jnp.dot(hidden_ref[...], down_ref[layer, 0, :, start:stop], preferred_element_type=jnp.float32)
        weighted = (part.astype(jnp.bfloat16).astype(jnp.float32) * gate).astype(jnp.bfloat16)
        for index, out in enumerate(outs):
            out[:, start:stop] = weighted[index * size : (index + 1) * size]
    sent = jnp.where(here & (block == 0), gate, 0.0)[:, model - tail :].astype(jnp.bfloat16)
    for index, out in enumerate(outs):
        out[:, model:] = sent[index * size : (index + 1) * size]


def expert_ffn(layer, pieces, router, up, down):
    count, width, units = len(pieces), pieces[0].shape[1], up.shape[2]
    total = sum(piece.shape[0] for piece in pieces)
    return pl.pallas_call(
        functools.partial(ffn_kernel, layer, count),
        out_shape=[jax.ShapeDtypeStruct((total // 8, width), jnp.bfloat16)] * 8,
        in_specs=[VMEM] * (count + 3),
        out_specs=[VMEM] * 8,
        scratch_shapes=[pltpu.VMEM((total, width), jnp.bfloat16), pltpu.VMEM((total, units), jnp.bfloat16)],
        compiler_params=pltpu.CompilerParams(vmem_limit_bytes=16 * 1024 * 1024),
        name=f"ffn_{layer}",
    )(*pieces, router, up, down)


def dense_moves(groups, columns):
    lengths = columns // 4

    def pairs(move):
        listed = []
        for group in range(groups):
            for far in range(lengths):
                for side in range(2):
                    for core in range(2):
                        to = move(group, far, side, core)
                        listed.append((((group * lengths + far) * 2 + side) * 2 + core, ((to[0] * lengths + to[1]) * 2 + to[2]) * 2 + to[3]))
        return listed

    def axis_swap(which):
        def move(group, far, side, core):
            return (group, far, 1 - side, core) if core == which else (1 - group, far, side, core)

        return pairs(move)

    def shift(amount):
        return pairs(lambda group, far, side, core: (group, far ^ amount, side, core))

    return lengths, shift, axis_swap(0), axis_swap(1), pairs(lambda group, far, side, core: (group, far, side, 1 - core))


def dense_device(tokens, routes, placement, up_weight, down_weight, router_weight):
    groups, columns = lax.axis_size("dp"), lax.axis_size("expert")
    layers, tok_rows, _ = routes.shape
    model = tokens.shape[1]
    width = round_up(model + columns, LANES)
    tail = model // LANES * LANES
    lengths, shift, first_swap, second_swap, core_swap = dense_moves(groups, columns)
    axes = ("dp", "expert")
    up_rows, router = jnp.swapaxes(up_weight, 2, 3), router_weight.reshape(layers, model)
    small = pltpu.CompilerParams(vmem_limit_bytes=4 * 1024 * 1024)
    payload_shape = jax.ShapeDtypeStruct((tok_rows, width), jnp.bfloat16)
    top_k, experts = routes.shape[2], placement.shape[1]
    lanes = max(tok_rows, experts)
    table = lax.pad(jnp.swapaxes(routes, 1, 2), 0, [(0, 0, 0), (0, 1, 0), (0, lanes - tok_rows, 0)]) + lax.pad(
        placement[:, None, :], 0, [(0, 0, 0), (top_k, 0, 0), (0, lanes - experts, 0)]
    )
    stream = tokens
    own, tails = pl.pallas_call(
        functools.partial(first_kernel, model, tail, experts),
        out_shape=[payload_shape, jax.ShapeDtypeStruct((layers, tok_rows, width - tail), jnp.float32)],
        in_specs=[VMEM] * 2,
        out_specs=[VMEM] * 2,
        compiler_params=small,
        cost_estimate=pl.CostEstimate(flops=20_000_000_000, transcendentals=0, bytes_accessed=0),
        name="first",
    )(tokens, table)

    wave = lengths // WAVES
    sequence = sorted(range(lengths), key=lambda step: (step % WAVES, step))

    def move(value, pairs):
        return lax.ppermute(value, axes, pairs)

    for layer in range(layers):
        line = [own] + [move(own, shift(step)) for step in range(1, lengths)]
        line = [line[step] for step in sequence]
        parts = [jnp.concatenate(line[start : start + wave], axis=0) for start in range(0, lengths, wave)]
        here = jnp.concatenate(line, axis=0)
        firsts = [move(part, first_swap) for part in parts]
        second = move(here, second_swap)
        acrosses = [move(part, second_swap) for part in firsts]
        near = [here, second] + firsts + acrosses
        outs = expert_ffn(layer, near + [move(piece, core_swap) for piece in near], router, up_rows, down_weight)
        here, second, first, across = [
            mine.astype(jnp.float32) + move(theirs, core_swap).astype(jnp.float32) for mine, theirs in zip(outs[:4], outs[4:])
        ]
        first = first + move(across.astype(jnp.bfloat16), second_swap).astype(jnp.float32)
        here = here + move(second.astype(jnp.bfloat16), second_swap).astype(jnp.float32)
        here = here + move(first.astype(jnp.bfloat16), first_swap).astype(jnp.float32)
        pieces = here.reshape(lengths, tok_rows, width)
        pieces = [pieces[sequence.index(step)] for step in range(lengths)]
        arrived = [move(pieces[step].astype(jnp.bfloat16), shift(step)) for step in range(1, lengths)]
        last = layer + 1 == layers
        outs = pl.pallas_call(
            functools.partial(update_kernel, model, tail, layer, last),
            out_shape=[jax.ShapeDtypeStruct(stream.shape, jnp.bfloat16)] + [payload_shape] * (not last),
            in_specs=[VMEM] * (len(arrived) + 3),
            out_specs=[VMEM] * (2 - last),
            compiler_params=small,
            name=f"update_{layer}",
        )(pieces[0], *arrived, stream, tails)
        stream, own = outs[0], outs[-1]
    return stream


def slot_table(route_rows, place_row, columns, capacity):
    tok_rows, top_k = route_rows.shape
    experts = place_row.shape[0]
    matches = route_rows[:, :, None] == jnp.arange(experts, dtype=jnp.int32)[None, None, :]
    target = jnp.sum(jnp.where(matches, place_row[None, None, :], 0), axis=2).reshape(-1)
    row_count = target.shape[0]
    positions = jnp.arange(row_count, dtype=jnp.int32)
    earlier = (positions[None, :] < positions[:, None]) & (target[None, :] == target[:, None])
    row_rank = jnp.sum(earlier.astype(jnp.int32), axis=1)
    placed = (target[:, None, None] == jnp.arange(columns, dtype=jnp.int32)[None, :, None]) & (
        row_rank[:, None, None] == jnp.arange(capacity, dtype=jnp.int32)[None, None, :]
    )
    slot_map = jnp.sum(
        placed.reshape(tok_rows, top_k, columns, capacity).astype(jnp.float32), axis=1
    )
    return jnp.transpose(slot_map, (1, 2, 0))


def dispatch_device(tokens, routes, placement, up_weight, down_weight, router_weight):
    groups = lax.axis_size("dp")
    columns = lax.axis_size("expert")
    tok_rows = tokens.shape[0]
    top_k = routes.shape[2]
    capacity = 2 * tok_rows * top_k // columns

    def layer_step(stream, packed):
        route_rows, place_row, up_part, down_part, router_part = packed
        normed = rms_rows(stream)
        slot_map = slot_table(route_rows, place_row, columns, capacity)
        outgoing = jnp.einsum(
            "jct,td->jcd", slot_map.astype(jnp.bfloat16), normed, preferred_element_type=jnp.float32
        ).astype(jnp.bfloat16)
        arrived = lax.all_to_all(
            outgoing, "expert", split_axis=0, concat_axis=0, tiled=True
        ).reshape(columns * capacity, -1)
        affinity = jax.nn.sigmoid(
            jnp.dot(arrived, router_part[0], preferred_element_type=jnp.float32)
        ).astype(jnp.bfloat16)
        all_rows, all_gates = (
            lax.all_gather(arrived, "dp", axis=0, tiled=True),
            lax.all_gather(affinity, "dp", axis=0, tiled=True),
        )
        hidden = jax.nn.silu(
            jnp.dot(all_rows, up_part[0], preferred_element_type=jnp.float32)
        ).astype(jnp.bfloat16)
        part_sums = jnp.dot(hidden, down_part[0], preferred_element_type=jnp.float32).astype(
            jnp.bfloat16
        )
        part_sums = part_sums.reshape(groups, columns, capacity, -1)
        all_gates = all_gates.reshape(groups, columns, capacity)
        returned, gates_back = (
            lax.all_to_all(
                lax.all_to_all(part_sums, "dp", split_axis=0, concat_axis=0, tiled=True),
                "expert",
                split_axis=1,
                concat_axis=1,
                tiled=True,
            ),
            lax.all_to_all(
                lax.all_to_all(all_gates, "dp", split_axis=0, concat_axis=0, tiled=True),
                "expert",
                split_axis=1,
                concat_axis=1,
                tiled=True,
            ),
        )
        weights = slot_map * gates_back[0].astype(jnp.float32)[:, :, None]
        numerator = jnp.einsum(
            "ect,gecd->td",
            weights.astype(jnp.bfloat16),
            returned,
            preferred_element_type=jnp.float32,
        )
        denominator = jnp.sum(weights, axis=(0, 1))
        updated = stream.astype(jnp.float32) + numerator / jnp.maximum(denominator, 0.5)[:, None]
        return (updated.astype(jnp.bfloat16), None)

    result_stream, unused = lax.scan(
        layer_step, tokens, (routes, placement, up_weight, down_weight, router_weight)
    )
    return result_stream


def per_device(tokens, routes, placement, up_weight, down_weight, router_weight):
    groups, columns = lax.axis_size("dp"), lax.axis_size("expert")
    tok_rows, top_k = tokens.shape[0], routes.shape[2]
    capacity = 2 * tok_rows * top_k // columns
    lengths = columns // 4
    dense = groups == 2 and columns == 4 * lengths and lengths & (lengths - 1) == 0 and lengths % WAVES == 0 and tok_rows <= 2 * capacity
    plan = dense_device if dense else dispatch_device
    return plan(tokens, routes, placement, up_weight, down_weight, router_weight)


def solution(mesh):
    return jax.shard_map(
        per_device,
        mesh=mesh,
        in_specs=(
            P(("dp", "expert"), None),
            P(None, ("dp", "expert"), None),
            P(),
            P(None, "expert", None, "dp"),
            P(None, "expert", "dp", None),
            P(None, "expert", None),
        ),
        out_specs=P(("dp", "expert"), None),
        check_vma=False,
    )
```

```python
import functools

import jax
import jax.numpy as jnp
from jax import lax
from jax.experimental import pallas as pl
from jax.experimental.pallas import tpu as pltpu
from jax.sharding import PartitionSpec as P

LANES = 128
WAVES = 2


def rms_rows(stream):
    values = stream.astype(jnp.float32)
    inverse = lax.rsqrt(jnp.mean(values * values, axis=-1, keepdims=True) + 1e-05)
    return (values * inverse).astype(jnp.bfloat16)


def round_up(value, unit):
    return -(-value // unit) * unit


VMEM = pl.BlockSpec(memory_space=pltpu.VMEM)
SMEM = pl.BlockSpec(memory_space=pltpu.SMEM)


def member_tail(layer, shift, lanes, tok_rows, experts, table_ref):
    top_k = table_ref.shape[1] - 1
    ids = lax.broadcasted_iota(jnp.int32, (experts, tok_rows), 0)
    named = jnp.zeros((experts, tok_rows), jnp.float32)
    for choice in range(top_k):
        named = jnp.where(ids == table_ref[layer, choice : choice + 1, :tok_rows], 1.0, named)
    lane = lax.broadcasted_iota(jnp.int32, (lanes, experts), 0)
    served = jnp.where(lane == table_ref[layer, top_k : top_k + 1, :experts] + shift, 1.0, 0.0)
    return lax.dot_general(named, served, (((0,), (1,)), ((), ())), preferred_element_type=jnp.float32)


def write_payload(values, tail_rows, model, tail, payload_ref):
    inverse = lax.rsqrt(jnp.mean(values * values, axis=-1, keepdims=True) + 1e-05)
    normed = (values * inverse).astype(jnp.bfloat16)
    payload_ref[:, :tail] = normed[:, :tail]
    payload_ref[:, tail:] = tail_rows.astype(jnp.bfloat16)
    if model > tail:
        payload_ref[:, tail:model] = normed[:, tail:]


def first_kernel(model, tail, experts, tokens_ref, table_ref, payload_ref, tails_ref):
    lanes = payload_ref.shape[1] - tail
    for layer in range(table_ref.shape[0]):
        tails_ref[layer] = member_tail(layer, model - tail, lanes, tokens_ref.shape[0], experts, table_ref)
    write_payload(tokens_ref[...].astype(jnp.float32), tails_ref[0], model, tail, payload_ref)


def update_kernel(model, tail, layer, last, own_ref, *refs):
    pieces, (stream_ref, tails_ref, updated_ref), more = refs[: len(refs) - 3 - (not last)], refs[len(refs) - 3 - (not last) :][:3], refs[len(refs) - (not last) :]
    total = own_ref[...]
    for piece in pieces:
        total = total + piece[...].astype(jnp.float32)
    denominator = jnp.maximum(jnp.sum(total[:, model:], axis=1, keepdims=True), 0.5)
    updated = (stream_ref[...].astype(jnp.float32) + total[:, :model] / denominator).astype(jnp.bfloat16)
    updated_ref[...] = updated
    if not last:
        write_payload(updated.astype(jnp.float32), tails_ref[layer + 1], model, tail, more[0])


def ffn_kernel(layer, count, *refs):
    pieces, (router_ref, up_ref, down_ref), outs, (rows_ref, hidden_ref) = refs[:count], refs[count : count + 3], refs[count + 3 : -2], refs[-2:]
    total, width = rows_ref.shape
    model, units = router_ref.shape[-1], up_ref.shape[2]
    size, filled = outs[0].shape[0], 0
    for piece in pieces:
        rows_ref[filled : filled + piece.shape[0], :] = piece[...]
        filled += piece.shape[0]
    slot, block = lax.axis_index("expert"), lax.axis_index("dp")
    tail = model // LANES * LANES
    lane = lax.broadcasted_iota(jnp.int32, (total, width - tail), 1)
    here = lane == (model - tail) + slot
    member = jnp.sum(jnp.where(here, rows_ref[:, tail:].astype(jnp.float32), 0.0), axis=1, keepdims=True)
    by_rows = (((1,), (1,)), ((), ()))
    logits = lax.dot_general(rows_ref[:, :model], router_ref[...], by_rows, preferred_element_type=jnp.float32)
    gate = jax.nn.sigmoid(logits[:, layer : layer + 1]).astype(jnp.bfloat16).astype(jnp.float32) * member
    for start in range(0, units, 256):
        stop = min(start + 256, units)
        raw = lax.dot_general(rows_ref[:, :model], up_ref[layer, 0, start:stop, :], by_rows, preferred_element_type=jnp.float32)
        hidden_ref[:, start:stop] = jax.nn.silu(raw).astype(jnp.bfloat16)
    for start in range(0, model, 768):
        stop = min(start + 768, model)
        part = jnp.dot(hidden_ref[...], down_ref[layer, 0, :, start:stop], preferred_element_type=jnp.float32)
        weighted = (part.astype(jnp.bfloat16).astype(jnp.float32) * gate).astype(jnp.bfloat16)
        for index, out in enumerate(outs):
            out[:, start:stop] = weighted[index * size : (index + 1) * size]
    sent = jnp.where(here & (block == 0), gate, 0.0)[:, model - tail :].astype(jnp.bfloat16)
    for index, out in enumerate(outs):
        out[:, model:] = sent[index * size : (index + 1) * size]


def expert_ffn(layer, pieces, router, up, down):
    count, width, units = len(pieces), pieces[0].shape[1], up.shape[2]
    total = sum(piece.shape[0] for piece in pieces)
    return pl.pallas_call(
        functools.partial(ffn_kernel, layer, count),
        out_shape=[jax.ShapeDtypeStruct((total // 8, width), jnp.bfloat16)] * 8,
        in_specs=[VMEM] * (count + 3),
        out_specs=[VMEM] * 8,
        scratch_shapes=[pltpu.VMEM((total, width), jnp.bfloat16), pltpu.VMEM((total, units), jnp.bfloat16)],
        compiler_params=pltpu.CompilerParams(vmem_limit_bytes=16 * 1024 * 1024),
        name=f"ffn_{layer}",
    )(*pieces, router, up, down)


def dense_moves(groups, columns):
    lengths = columns // 4

    def pairs(move):
        listed = []
        for group in range(groups):
            for far in range(lengths):
                for side in range(2):
                    for core in range(2):
                        to = move(group, far, side, core)
                        listed.append((((group * lengths + far) * 2 + side) * 2 + core, ((to[0] * lengths + to[1]) * 2 + to[2]) * 2 + to[3]))
        return listed

    def axis_swap(which):
        def move(group, far, side, core):
            return (group, far, 1 - side, core) if core == which else (1 - group, far, side, core)

        return pairs(move)

    def shift(amount):
        return pairs(lambda group, far, side, core: (group, far ^ amount, side, core))

    return lengths, shift, axis_swap(0), axis_swap(1), pairs(lambda group, far, side, core: (group, far, side, 1 - core))


def dense_device(tokens, routes, placement, up_weight, down_weight, router_weight):
    groups, columns = lax.axis_size("dp"), lax.axis_size("expert")
    layers, tok_rows, _ = routes.shape
    model = tokens.shape[1]
    width = round_up(model + columns, LANES)
    tail = model // LANES * LANES
    lengths, shift, first_swap, second_swap, core_swap = dense_moves(groups, columns)
    axes = ("dp", "expert")
    up_rows, router = jnp.swapaxes(up_weight, 2, 3), router_weight.reshape(layers, model)
    small = pltpu.CompilerParams(vmem_limit_bytes=4 * 1024 * 1024)
    payload_shape = jax.ShapeDtypeStruct((tok_rows, width), jnp.bfloat16)
    top_k, experts = routes.shape[2], placement.shape[1]
    lanes = max(tok_rows, experts)
    table = lax.pad(jnp.swapaxes(routes, 1, 2), 0, [(0, 0, 0), (0, 1, 0), (0, lanes - tok_rows, 0)]) + lax.pad(
        placement[:, None, :], 0, [(0, 0, 0), (top_k, 0, 0), (0, lanes - experts, 0)]
    )
    stream = tokens
    own, tails = pl.pallas_call(
        functools.partial(first_kernel, model, tail, experts),
        out_shape=[payload_shape, jax.ShapeDtypeStruct((layers, tok_rows, width - tail), jnp.float32)],
        in_specs=[VMEM] * 2,
        out_specs=[VMEM] * 2,
        compiler_params=small,
        cost_estimate=pl.CostEstimate(flops=20_000_000_000, transcendentals=0, bytes_accessed=0),
        name="first",
    )(tokens, table)

    wave = lengths // WAVES
    sequence = sorted(range(lengths), key=lambda step: (step % WAVES, step))

    def move(value, pairs):
        return lax.ppermute(value, axes, pairs)

    for layer in range(layers):
        line = [own] + [move(own, shift(step)) for step in range(1, lengths)]
        line = [line[step] for step in sequence]
        parts = [jnp.concatenate(line[start : start + wave], axis=0) for start in range(0, lengths, wave)]
        here = jnp.concatenate(line, axis=0)
        firsts = [move(part, first_swap) for part in parts]
        second = move(here, second_swap)
        acrosses = [move(part, second_swap) for part in firsts]
        near = [here, second] + firsts + acrosses
        outs = expert_ffn(layer, near + [move(piece, core_swap) for piece in near], router, up_rows, down_weight)
        here, second, first, across = [
            mine.astype(jnp.float32) + move(theirs, core_swap).astype(jnp.float32) for mine, theirs in zip(outs[:4], outs[4:])
        ]
        first = first + move(across.astype(jnp.bfloat16), second_swap).astype(jnp.float32)
        side = move(second.astype(jnp.bfloat16), second_swap).astype(jnp.float32)
        here = here + (side + move(first.astype(jnp.bfloat16), first_swap).astype(jnp.float32))
        pieces = here.reshape(lengths, tok_rows, width)
        pieces = [pieces[sequence.index(step)] for step in range(lengths)]
        arrived = [move(pieces[step].astype(jnp.bfloat16), shift(step)) for step in range(1, lengths)]
        last = layer + 1 == layers
        outs = pl.pallas_call(
            functools.partial(update_kernel, model, tail, layer, last),
            out_shape=[jax.ShapeDtypeStruct(stream.shape, jnp.bfloat16)] + [payload_shape] * (not last),
            in_specs=[VMEM] * (len(arrived) + 3),
            out_specs=[VMEM] * (2 - last),
            compiler_params=small,
            name=f"update_{layer}",
        )(pieces[0], *arrived, stream, tails)
        stream, own = outs[0], outs[-1]
    return stream


def slot_table(route_rows, place_row, columns, capacity):
    tok_rows, top_k = route_rows.shape
    experts = place_row.shape[0]
    matches = route_rows[:, :, None] == jnp.arange(experts, dtype=jnp.int32)[None, None, :]
    target = jnp.sum(jnp.where(matches, place_row[None, None, :], 0), axis=2).reshape(-1)
    row_count = target.shape[0]
    positions = jnp.arange(row_count, dtype=jnp.int32)
    earlier = (positions[None, :] < positions[:, None]) & (target[None, :] == target[:, None])
    row_rank = jnp.sum(earlier.astype(jnp.int32), axis=1)
    placed = (target[:, None, None] == jnp.arange(columns, dtype=jnp.int32)[None, :, None]) & (
        row_rank[:, None, None] == jnp.arange(capacity, dtype=jnp.int32)[None, None, :]
    )
    slot_map = jnp.sum(
        placed.reshape(tok_rows, top_k, columns, capacity).astype(jnp.float32), axis=1
    )
    return jnp.transpose(slot_map, (1, 2, 0))


def dispatch_device(tokens, routes, placement, up_weight, down_weight, router_weight):
    groups = lax.axis_size("dp")
    columns = lax.axis_size("expert")
    tok_rows = tokens.shape[0]
    top_k = routes.shape[2]
    capacity = 2 * tok_rows * top_k // columns

    def layer_step(stream, packed):
        route_rows, place_row, up_part, down_part, router_part = packed
        normed = rms_rows(stream)
        slot_map = slot_table(route_rows, place_row, columns, capacity)
        outgoing = jnp.einsum(
            "jct,td->jcd", slot_map.astype(jnp.bfloat16), normed, preferred_element_type=jnp.float32
        ).astype(jnp.bfloat16)
        arrived = lax.all_to_all(
            outgoing, "expert", split_axis=0, concat_axis=0, tiled=True
        ).reshape(columns * capacity, -1)
        affinity = jax.nn.sigmoid(
            jnp.dot(arrived, router_part[0], preferred_element_type=jnp.float32)
        ).astype(jnp.bfloat16)
        all_rows, all_gates = (
            lax.all_gather(arrived, "dp", axis=0, tiled=True),
            lax.all_gather(affinity, "dp", axis=0, tiled=True),
        )
        hidden = jax.nn.silu(
            jnp.dot(all_rows, up_part[0], preferred_element_type=jnp.float32)
        ).astype(jnp.bfloat16)
        part_sums = jnp.dot(hidden, down_part[0], preferred_element_type=jnp.float32).astype(
            jnp.bfloat16
        )
        part_sums = part_sums.reshape(groups, columns, capacity, -1)
        all_gates = all_gates.reshape(groups, columns, capacity)
        returned, gates_back = (
            lax.all_to_all(
                lax.all_to_all(part_sums, "dp", split_axis=0, concat_axis=0, tiled=True),
                "expert",
                split_axis=1,
                concat_axis=1,
                tiled=True,
            ),
            lax.all_to_all(
                lax.all_to_all(all_gates, "dp", split_axis=0, concat_axis=0, tiled=True),
                "expert",
                split_axis=1,
                concat_axis=1,
                tiled=True,
            ),
        )
        weights = slot_map * gates_back[0].astype(jnp.float32)[:, :, None]
        numerator = jnp.einsum(
            "ect,gecd->td",
            weights.astype(jnp.bfloat16),
            returned,
            preferred_element_type=jnp.float32,
        )
        denominator = jnp.sum(weights, axis=(0, 1))
        updated = stream.astype(jnp.float32) + numerator / jnp.maximum(denominator, 0.5)[:, None]
        return (updated.astype(jnp.bfloat16), None)

    result_stream, unused = lax.scan(
        layer_step, tokens, (routes, placement, up_weight, down_weight, router_weight)
    )
    return result_stream


def per_device(tokens, routes, placement, up_weight, down_weight, router_weight):
    groups, columns = lax.axis_size("dp"), lax.axis_size("expert")
    tok_rows, top_k = tokens.shape[0], routes.shape[2]
    capacity = 2 * tok_rows * top_k // columns
    lengths = columns // 4
    dense = groups == 2 and columns == 4 * lengths and lengths & (lengths - 1) == 0 and lengths % WAVES == 0 and tok_rows <= 2 * capacity
    plan = dense_device if dense else dispatch_device
    return plan(tokens, routes, placement, up_weight, down_weight, router_weight)


def solution(mesh):
    return jax.shard_map(
        per_device,
        mesh=mesh,
        in_specs=(
            P(("dp", "expert"), None),
            P(None, ("dp", "expert"), None),
            P(),
            P(None, "expert", None, "dp"),
            P(None, "expert", "dp", None),
            P(None, "expert", None),
        ),
        out_specs=P(("dp", "expert"), None),
        check_vma=False,
    )
```
